128 devices in a mesh: tp: 2 (over core), dp: 64 (over z, y, x).
Axes of the slice: x: 4, y: 4, z: 4, core: 2. Of those that a mesh axis runs over, the one named last changes fastest.
Arguments:
- x_tokens: bfloat16 [16384, 2048], P('dp')
- dh_out: bfloat16 [16384, 2048], P('dp')
- w_in: bfloat16 [2, 2048, 8192], P(None, None, 'tp')
- w_out: bfloat16 [2, 8192, 2048], P(None, 'tp')
- p_in: bfloat16 [2, 2048, 256], replicated
- q_out: bfloat16 [2, 2048, 256], replicated
- m_in: float32 [2, 256, 8192], P(None, None, ('tp', 'dp'))
- v_in: float32 [2, 256, 8192], P(None, None, ('tp', 'dp'))
- m_out: float32 [2, 8192, 256], P(None, ('tp', 'dp'))
- v_out: float32 [2, 8192, 256], P(None, ('tp', 'dp'))
Outputs:
- output 1: bfloat16 [2, 2048, 8192], P(None, None, 'tp')
- output 2: bfloat16 [2, 8192, 2048], P(None, 'tp')
- output 3: float32 [2, 256, 8192], P(None, None, ('tp', 'dp'))
- output 4: float32 [2, 256, 8192], P(None, None, ('tp', 'dp'))
- output 5: float32 [2, 8192, 256], P(None, ('tp', 'dp'))
- output 6: float32 [2, 8192, 256], P(None, ('tp', 'dp'))
All inputs are finite; a program needn't handle non-finite values.
Results may differ from the reference program's by a relative error of at most 0.0108964.
Values are sent between devices in bfloat16 or wider.
A program may use at most 1 GiB of HBM per device.

```python
import jax
import jax.numpy as jnp
from jax import lax

D = 2048
FF = 8192
RANK = 256
TOKENS = 16384
ROW_BLOCK = 256
LAYERS = 2
STEP = 2

BETA1 = 0.9
BETA2 = 0.999
EPSILON = 1e-8
STEP_SIZE = 0.03 * 0.25
CORR_MOM = 1.0 - BETA1 ** STEP
CORR_VAR = 1.0 - BETA2 ** STEP


def setup_inputs(seed: int = 0) -> dict:
    rng_keys = jax.random.split(jax.random.key(seed), 10)
    grad_scale = 0.5 * TOKENS ** 0.5
    x_tokens = jax.random.normal(rng_keys[0], (TOKENS, D), jnp.float32)
    dh_out = jax.random.normal(rng_keys[1], (TOKENS, D), jnp.float32)
    w_in = jax.random.normal(rng_keys[2], (LAYERS, D, FF), jnp.float32) * D ** -0.5
    w_out = jax.random.normal(rng_keys[3], (LAYERS, FF, D), jnp.float32) * FF ** -0.5
    p_in = jax.random.normal(rng_keys[4], (LAYERS, D, RANK), jnp.float32) * D ** -0.5
    q_out = jax.random.normal(rng_keys[5], (LAYERS, D, RANK), jnp.float32) * D ** -0.5
    m_in = jax.random.normal(rng_keys[6], (LAYERS, RANK, FF), jnp.float32) * ((1.0 - BETA1) * grad_scale)
    v_in = (jax.random.normal(rng_keys[7], (LAYERS, RANK, FF), jnp.float32) ** 2 + 0.25) * ((1.0 - BETA2) * grad_scale ** 2)
    m_out = jax.random.normal(rng_keys[8], (LAYERS, FF, RANK), jnp.float32) * ((1.0 - BETA1) * grad_scale)
    v_out = (jax.random.normal(rng_keys[9], (LAYERS, FF, RANK), jnp.float32) ** 2 + 0.25) * ((1.0 - BETA2) * grad_scale ** 2)
    return {"x_tokens": x_tokens.astype(jnp.bfloat16), "dh_out": dh_out.astype(jnp.bfloat16), "w_in": w_in.astype(jnp.bfloat16), "w_out": w_out.astype(jnp.bfloat16), "p_in": p_in.astype(jnp.bfloat16), "q_out": q_out.astype(jnp.bfloat16), "m_in": m_in, "v_in": v_in, "m_out": m_out, "v_out": v_out}


def adam_direction(grad_proj, moment, second):
    moment_new = BETA1 * moment + (1.0 - BETA1) * grad_proj
    second_new = BETA2 * second + (1.0 - BETA2) * grad_proj * grad_proj
    direction = (moment_new / CORR_MOM) / (jnp.sqrt(second_new / CORR_VAR) + EPSILON)
    return direction.astype(jnp.bfloat16), moment_new, second_new


def reference(x_tokens, dh_out, w_in, w_out, p_in, q_out, m_in, v_in, m_out, v_out):
    def row_block(grad_acc, row_pair):
        x_rows, g_rows = row_pair
        states = [x_rows]
        activations = []
        gelu_vjps = []
        for layer_idx in range(LAYERS):
            pre_act = jnp.dot(states[-1], w_in[layer_idx], preferred_element_type=jnp.float32).astype(jnp.bfloat16)
            act_f32, gelu_vjp = jax.vjp(jax.nn.gelu, pre_act.astype(jnp.float32))
            act_bf16 = act_f32.astype(jnp.bfloat16)
            activations.append(act_bf16)
            gelu_vjps.append(gelu_vjp)
            if layer_idx < LAYERS - 1:
                mlp_out = jnp.dot(act_bf16, w_out[layer_idx], preferred_element_type=jnp.float32)
                states.append((states[-1].astype(jnp.float32) + mlp_out).astype(jnp.bfloat16))
        grads_in = list(grad_acc[0])
        grads_out = list(grad_acc[1])
        cotangent = g_rows
        for layer_idx in reversed(range(LAYERS)):
            grads_out[layer_idx] = grads_out[layer_idx] + jnp.dot(activations[layer_idx].T, cotangent, preferred_element_type=jnp.float32)
            d_act = jnp.dot(cotangent, w_out[layer_idx].T, preferred_element_type=jnp.float32)
            d_pre = gelu_vjps[layer_idx](d_act)[0].astype(jnp.bfloat16)
            grads_in[layer_idx] = grads_in[layer_idx] + jnp.dot(states[layer_idx].T, d_pre, preferred_element_type=jnp.float32)
            if layer_idx > 0:
                back_sum = jnp.dot(d_pre, w_in[layer_idx].T, preferred_element_type=jnp.float32)
                cotangent = (cotangent.astype(jnp.float32) + back_sum).astype(jnp.bfloat16)
        return (tuple(grads_in), tuple(grads_out)), None

    blocks = TOKENS // ROW_BLOCK
    x_blocks = x_tokens.reshape(blocks, ROW_BLOCK, D)
    g_blocks = dh_out.reshape(blocks, ROW_BLOCK, D)
    zeros_in = tuple(jnp.zeros((D, FF), jnp.float32) for layer_idx in range(LAYERS))
    zeros_out = tuple(jnp.zeros((FF, D), jnp.float32) for layer_idx in range(LAYERS))
    (grads_in, grads_out), _unused = lax.scan(row_block, (zeros_in, zeros_out), (x_blocks, g_blocks))
    results = [[], [], [], [], [], []]
    for layer_idx in range(LAYERS):
        proj_in = jnp.dot(p_in[layer_idx].astype(jnp.float32).T, grads_in[layer_idx], precision=lax.Precision.HIGHEST)
        proj_out = jnp.dot(grads_out[layer_idx], q_out[layer_idx].astype(jnp.float32), precision=lax.Precision.HIGHEST)
        dir_in, mom_in, var_in = adam_direction(proj_in, m_in[layer_idx], v_in[layer_idx])
        dir_out, mom_out, var_out = adam_direction(proj_out, m_out[layer_idx], v_out[layer_idx])
        upd_in = jnp.dot(p_in[layer_idx], dir_in, preferred_element_type=jnp.float32)
        upd_out = jnp.dot(dir_out, q_out[layer_idx].T, preferred_element_type=jnp.float32)
        results[0].append((w_in[layer_idx].astype(jnp.float32) - STEP_SIZE * upd_in).astype(jnp.bfloat16))
        results[1].append((w_out[layer_idx].astype(jnp.float32) - STEP_SIZE * upd_out).astype(jnp.bfloat16))
        results[2].append(mom_in)
        results[3].append(var_in)
        results[4].append(mom_out)
        results[5].append(var_out)
    return (jnp.stack(results[0]), jnp.stack(results[1]), jnp.stack(results[2]), jnp.stack(results[3]), jnp.stack(results[4]), jnp.stack(results[5]))
```

```python
import functools

import jax
import jax.numpy as jnp
from jax import lax
from jax.experimental import pallas as pl
from jax.experimental.pallas import tpu as pltpu
from jax.sharding import PartitionSpec as P

BETA1 = 0.9
BETA2 = 0.999
EPSILON = 1e-8
STEP = 2
STEP_SIZE = 0.03 * 0.25
CORR_MOM = 1.0 - BETA1 ** STEP
CORR_VAR = 1.0 - BETA2 ** STEP

MESH = pl.DeviceIdType.MESH
BF16 = jnp.bfloat16
F32 = jnp.float32

TOK = 256
D = 2048
F = 4096
RANK = 256
DP = 64
TILE = 512
CHUNKS = 8
SLOTS = 4
DIMS = 6
COLORS = 3

CUTS = (((0, 3, 6, 8), (0, 2, 4, 8)), ((0, 3, 6, 8), (0, 3, 5, 8)))
BLOCKS = tuple(
    tuple(
        tuple((tensor, block) for tensor, cut in enumerate(cuts) for block in range(cut[color], cut[color + 1]))
        for color in range(COLORS)
    )
    for cuts in CUTS
)
WHERE = tuple(
    {item: (color, slot) for color, items in enumerate(colors) for slot, item in enumerate(items)} for colors in BLOCKS
)
FIRST_PART = tuple(CUTS[0][0][color + 1] - CUTS[0][0][color] for color in range(COLORS))


def ring_bits(position):
    high = lax.div(position, 2)
    return [lax.rem(high + position, 2), high]


def device_bits(dp):
    return ring_bits(lax.rem(dp, 4)) + ring_bits(lax.rem(lax.div(dp, 4), 4)) + ring_bits(lax.div(dp, 16))


def step_bits(tile, lane):
    x = lane % 4
    odd = lax.rem(tile, 2)
    y_low = odd if lane < 4 else 1 - odd
    z_high = lax.div(tile, 4)
    z_low = lax.rem(z_high + lax.rem(lax.div(tile, 2), 2), 2)
    return [(x // 2 + x) % 2, x // 2, y_low, odd, z_low, z_high]


def stage_dim(color, stage, core):
    return (2 * color + core + stage) % DIMS


def place(bits, color, tp):
    at = [sum(bits[stage_dim(color, stage, core)] * (32 >> stage) for stage in range(DIMS)) for core in range(2)]
    return at[0] * (1 - tp) + at[1] * tp


def flip(dp, dim):
    stride = 4 ** (dim // 2)
    position = lax.rem(lax.div(dp, stride), 4)
    other = 3 - position if dim % 2 else position + 1 - 2 * lax.rem(position, 2)
    return dp + (other - position) * stride


def by_core(tp, function, color, stage):
    zero, one = (function(stage_dim(color, stage, core)) for core in range(2))
    return zero * (1 - tp) + one * tp


def dot(left, right, left_dim=1, right_dim=0):
    return lax.dot_general(left, right, (((left_dim,), (right_dim,)), ((), ())), preferred_element_type=F32)


GELU_A = 0.7978845608028654
GELU_B = 0.044715


def gelu(z):
    return 0.5 * z * (1.0 + jnp.tanh(GELU_A * (z + GELU_B * z * z * z)))


def gelu_grad(z):
    square = z * z
    t = jnp.tanh(GELU_A * (z + GELU_B * z * square))
    return 0.5 * (1.0 + t) + 0.5 * z * (1.0 - t * t) * (GELU_A * (1.0 + 3.0 * GELU_B * square))


def step_kernel(x_hbm, g_hbm, w_in, w_out, p_in, q_out, m_ref, v_ref, *rest):
    rest = iter(rest)

    def by_group():
        return tuple(tuple(next(rest) for color in range(COLORS)) for group in range(2))

    n_out = by_group()
    m_new, v_new = next(rest), next(rest)
    red, got, gat = by_group(), by_group(), by_group()
    (h_buf, g_buf, a_buf, z0_buf, z1_buf, w_buf, pq_buf, hp0, gq1, hp1, gq0,
     w_sem, in_sem, pq_sem, out_sem, pair_send, pair_recv, send_sem, recv_sem) = rest
    dp = lax.axis_index("dp")
    tp = lax.axis_index("tp")
    bits = device_bits(dp)

    barrier = pltpu.get_barrier_semaphore()
    for dim in range(DIMS):
        pl.semaphore_signal(barrier, inc=1, device_id={"dp": flip(dp, dim)}, device_id_type=MESH)
    pl.semaphore_signal(barrier, inc=1, device_id={"tp": 1 - tp}, device_id_type=MESH)
    pl.semaphore_wait(barrier, DIMS + 1)

    def block_of(phase, chunk, q):
        name, layer = phase
        half, rest_ = lax.rem(chunk, 2), lax.div(chunk, 2)
        if name == "z":
            return w_in.at[layer, pl.ds(TILE * q, TILE), pl.ds(pl.multiple_of(TILE * chunk, TILE), TILE)]
        if name == "h":
            return w_out.at[layer, pl.ds(pl.multiple_of(2048 * half, TILE) + TILE * q, TILE),
                            pl.ds(pl.multiple_of(TILE * rest_, TILE), TILE)]
        if name == "da":
            return w_out.at[layer, pl.ds(pl.multiple_of(TILE * chunk, TILE), TILE), pl.ds(TILE * q, TILE)]
        return w_in.at[layer, pl.ds(pl.multiple_of(TILE * rest_, TILE), TILE),
                       pl.ds(pl.multiple_of(2048 * half + TILE * q, TILE), TILE)]

    def start_chunk(phase, chunk):
        slot = lax.rem(chunk, SLOTS)
        for q in range(4):
            pltpu.make_async_copy(block_of(phase, chunk, q), w_buf.at[slot, q], w_sem.at[slot]).start()

    def wait_chunk(chunk):
        slot = lax.rem(chunk, SLOTS)
        pltpu.make_async_copy(w_buf.at[slot], w_buf.at[slot], w_sem.at[slot]).wait()
        return slot

    phases = (("z", 0), ("h", 0), ("z", 1), ("da", 1), ("b", 1), ("da", 0))

    def take_chunk(index, chunk):
        ahead = chunk + SLOTS - 1

        @pl.when(ahead < CHUNKS)
        def _():
            start_chunk(phases[index], ahead)

        if index + 1 < len(phases):

            @pl.when(ahead >= CHUNKS)
            def _():
                start_chunk(phases[index + 1], ahead - CHUNKS)

        return wait_chunk(chunk)

    def load_pq(ref, layer, slot):
        pltpu.make_async_copy(ref.at[layer], pq_buf.at[slot], pq_sem.at[slot]).start()

    def wait_pq(ref, slot):
        pltpu.make_async_copy(ref.at[0], pq_buf.at[slot], pq_sem.at[slot]).wait()

    x_copy = pltpu.make_async_copy(x_hbm, h_buf, in_sem.at[0])
    g_copy = pltpu.make_async_copy(g_hbm, g_buf, in_sem.at[1])
    x_copy.start()
    for chunk in range(SLOTS - 1):
        start_chunk(phases[0], jnp.int32(chunk))
    g_copy.start()
    load_pq(p_in, 0, 0)
    load_pq(q_out, 1, 1)

    def split(values, out_ref):
        high = values.astype(BF16)
        rest_ = values - high.astype(F32)
        middle = rest_.astype(BF16)
        low = (rest_ - middle.astype(F32)).astype(BF16)
        out_ref[:, 0:RANK] = high
        out_ref[:, RANK : 2 * RANK] = middle
        out_ref[:, 2 * RANK : 3 * RANK] = low

    def project(rows, parts, group, tensor, tile):
        wide = dot(rows, parts[...], 0, 0)
        total = wide[:, 2 * RANK : 3 * RANK] + wide[:, RANK : 2 * RANK] + wide[:, 0:RANK]
        for lane in range(8):
            lane_bits = step_bits(tile, lane)
            spots = [place(lane_bits, color, tp) for color in range(COLORS)]
            for block in range(8):
                color, slot = WHERE[group][tensor, block]
                row, col = 64 * lane + 16 * (block // 2), 128 * (block % 2)
                red[group][color][slot, spots[color]] = total[row : row + 16, col : col + 128]

    def columns(tile):
        return pl.ds(pl.multiple_of(TILE * tile, TILE), TILE)

    def pair_copy(exchange, n):
        return pltpu.make_async_remote_copy(
            src_ref=red[1][0].at[n], dst_ref=red[1][1 + exchange].at[n],
            send_sem=pair_send.at[exchange, n], recv_sem=pair_recv.at[exchange, n],
            device_id={"tp": 1 - tp}, device_id_type=MESH)

    def pair_send_tile(exchange, n, values):
        for a in range(16):
            for b in range(4):
                red[1][0][n, 4 * a + b] = values[16 * a : 16 * a + 16, 128 * b : 128 * b + 128]
        pair_copy(exchange, n).start()

    def pair_add(exchange, state):
        def one(n, carry):
            pair_copy(exchange, n).wait()
            for a in range(16):
                for b in range(4):
                    cols = pl.ds(pl.multiple_of(TILE * n + 128 * b, 128), 128)
                    both = red[1][0][n, 4 * a + b] + red[1][1 + exchange][n, 4 * a + b]
                    state[16 * a : 16 * a + 16, cols] = (
                        state[16 * a : 16 * a + 16, cols].astype(F32) + both).astype(BF16)
            return carry

        lax.fori_loop(0, 4, one, 0)

    own = [place(bits, color, tp) for color in range(COLORS)]

    def message(group, color, number, source, target, dim_stage):
        return pltpu.make_async_remote_copy(
            src_ref=source, dst_ref=target,
            send_sem=send_sem.at[group, color, number], recv_sem=recv_sem.at[group, color, number],
            device_id={"dp": by_core(tp, functools.partial(flip, dp), color, dim_stage)}, device_id_type=MESH)

    def start_of(color, stage):
        width = DP >> stage
        return lax.div(own[color], width) * width

    def reduce_copy(group, color, stage, part, parts, slots=None):
        half = 32 >> stage
        size = half // parts
        mine = lax.rem(lax.div(own[color], half), 2)
        source = start_of(color, stage) + (1 - mine) * half + part * size
        target = DP - (DP >> stage) + part * size
        slots = slice(None) if slots is None else slots
        number = (part if slots == slice(None) else (0 if slots.start == 0 else 1)) if stage == 0 else (
            4 + part if stage == 1 else 4 + stage)
        return message(group, color, number, red[group][color].at[slots, pl.ds(source, size)],
                       got[group][color].at[slots, pl.ds(target, size)], stage)

    def reduce_part(group, color, stage, part, parts):
        if group == 0 and stage == 0:
            first = FIRST_PART[color]
            return reduce_copy(group, color, 0, 0, 1, slice(first, len(BLOCKS[0][color])) if part else slice(0, first))
        return reduce_copy(group, color, stage, part, parts)

    def reduce_send(group, stage, parts=1, part=0):
        for color in range(COLORS):
            reduce_part(group, color, stage, part, parts).start()

    def reduce_add(group, stage, parts=1):
        half = 32 >> stage
        step = min(half, 4)
        for color in range(COLORS):
            for part in range(2 if group == 0 and stage == 0 else parts):
                reduce_part(group, color, stage, part, parts).wait()
            kept = start_of(color, stage + 1)
            offset = DP - (DP >> stage)

            def one(i, carry):
                for slot in range(len(BLOCKS[group][color])):
                    to = pl.ds(kept + step * i, step)
                    red[group][color][slot, to] = (
                        red[group][color][slot, to] + got[group][color][slot, pl.ds(offset + step * i, step)])
                return carry

            lax.fori_loop(0, half // step, one, 0)

    def update(group):
        for color in range(COLORS):
            for slot, (tensor, block) in enumerate(BLOCKS[group][color]):
                row, col = 16 * (block // 2), 128 * (block % 2)
                spot = (2 * group + tensor, slice(row, row + 16), slice(col, col + 128))
                grad = red[group][color][slot, own[color]]
                moment = BETA1 * m_ref[spot] + (1.0 - BETA1) * grad
                second = BETA2 * v_ref[spot] + (1.0 - BETA2) * grad * grad
                m_new[spot] = moment
                v_new[spot] = second
                direction = (moment / CORR_MOM) / (jnp.sqrt(second / CORR_VAR) + EPSILON)
                gat[group][color][slot, own[color]] = direction.astype(BF16)

    def gather_copy(group, color, turn, part, parts):
        stage = DIMS - 1 - turn
        size = (1 << turn) // parts
        spot = pl.ds(start_of(color, stage + 1) + part * size, size)
        number = 10 + turn + part
        return message(group, color, number, gat[group][color].at[:, spot], gat[group][color].at[:, spot], stage)

    def gather_send(group, turn, parts=1, part=0):
        for color in range(COLORS):
            gather_copy(group, color, turn, part, parts).start()

    def gather_wait(group, turn, parts=1):
        for color in range(COLORS):
            for part in range(parts):
                gather_copy(group, color, turn, part, parts).wait()

    def write_out(group, wait=False):
        for color in range(COLORS):
            copy = pltpu.make_async_copy(gat[group][color], n_out[group][color], out_sem.at[group, color])
            copy.wait() if wait else copy.start()

    x_copy.wait()

    def z0_step(tile, carry):
        slot = take_chunk(0, tile)
        z = sum(dot(h_buf[:, TILE * q : TILE * (q + 1)], w_buf[slot, q]) for q in range(4)).astype(BF16)
        z0_buf[:, columns(tile)] = z
        a_buf[:, columns(tile)] = gelu(z.astype(F32)).astype(BF16)
        return carry

    lax.fori_loop(0, CHUNKS, z0_step, 0)

    def h_step(n, carry):
        total = None
        for half in range(2):
            slot = take_chunk(1, 2 * n + half)
            for q in range(4):
                at = 2048 * half + TILE * q
                term = dot(a_buf[:, at : at + TILE], w_buf[slot, q])
                total = term if total is None else total + term
        pair_send_tile(0, n, total)
        return carry

    lax.fori_loop(0, 4, h_step, 0)
    wait_pq(p_in, 0)
    split(dot(h_buf[...], pq_buf[0]), hp0)
    load_pq(p_in, 1, 0)
    g_copy.wait()
    wait_pq(q_out, 1)
    split(dot(g_buf[...], pq_buf[1]), gq1)
    load_pq(q_out, 0, 1)
    pair_add(0, h_buf)

    def z1_step(tile, carry):
        slot = take_chunk(2, tile)
        z = sum(dot(h_buf[:, TILE * q : TILE * (q + 1)], w_buf[slot, q]) for q in range(4)).astype(BF16)
        z1_buf[:, columns(tile)] = z
        project(gelu(z.astype(F32)).astype(BF16), gq1, 0, 0, tile)
        return carry

    lax.fori_loop(0, CHUNKS, z1_step, 0)
    reduce_send(0, 0, part=0)
    wait_pq(p_in, 0)
    split(dot(h_buf[...], pq_buf[0]), hp1)

    def da1_step(tile, carry):
        slot = take_chunk(3, tile)
        d_act = sum(dot(g_buf[:, TILE * q : TILE * (q + 1)], w_buf[slot, q], 1, 1) for q in range(4))
        dz = (gelu_grad(z1_buf[:, columns(tile)].astype(F32)) * d_act).astype(BF16)
        z1_buf[:, columns(tile)] = dz
        project(dz, hp1, 0, 1, tile)
        return carry

    lax.fori_loop(0, CHUNKS, da1_step, 0)
    reduce_send(0, 0, part=1)

    def b_step(n, carry):
        total = None
        for half in range(2):
            slot = take_chunk(4, 2 * n + half)
            for q in range(4):
                at = 2048 * half + TILE * q
                term = dot(z1_buf[:, at : at + TILE], w_buf[slot, q], 1, 1)
                total = term if total is None else total + term
        pair_send_tile(1, n, total)
        return carry

    lax.fori_loop(0, 4, b_step, 0)
    wait_pq(q_out, 1)
    pair_add(1, g_buf)
    split(dot(g_buf[...], pq_buf[1]), gq0)

    def da0_step(tile, carry):
        slot = take_chunk(5, tile)
        project(a_buf[:, columns(tile)], gq0, 1, 0, tile)
        d_act = sum(dot(g_buf[:, TILE * q : TILE * (q + 1)], w_buf[slot, q], 1, 1) for q in range(4))
        dz = (gelu_grad(z0_buf[:, columns(tile)].astype(F32)) * d_act).astype(BF16)
        project(dz, hp0, 1, 1, tile)
        return carry

    lax.fori_loop(0, CHUNKS, da0_step, 0)

    for stage in range(4):
        reduce_add(0, stage)
        reduce_send(0, stage + 1)
        reduce_send(1, 0, 4, stage)
    reduce_add(0, 4)
    reduce_send(0, 5)
    reduce_add(1, 0, 4)
    reduce_send(1, 1, 2, 0)
    reduce_add(0, 5)
    update(0)
    gather_send(0, 0)
    reduce_send(1, 1, 2, 1)
    gather_wait(0, 0)
    gather_send(0, 1)
    for stage in range(1, 5):
        reduce_add(1, stage, 2 if stage == 1 else 1)
        reduce_send(1, stage + 1)
        gather_wait(0, stage)
        if stage < 4:
            gather_send(0, stage + 1)
    gather_send(0, 5, 4, 0)
    reduce_add(1, 5)
    update(1)
    gather_send(1, 0)
    gather_send(0, 5, 4, 1)
    for turn in range(2):
        gather_wait(1, turn)
        gather_send(1, turn + 1)
        gather_send(0, 5, 4, 2 + turn)
    for turn in range(2, 5):
        gather_wait(1, turn)
        gather_send(1, turn + 1)
        if turn == 3:
            gather_wait(0, 5, 4)
            write_out(0)
    gather_wait(1, 5)
    write_out(1)
    write_out(0, wait=True)
    write_out(1, wait=True)


def apply_kernel(order, w_in, w_out, p_in, q_out, *rest):
    gat = (rest[0:3], rest[3:6])
    in_new, out_new, n_buf = rest[6:9]
    layer = order - 1 - pl.program_id(0)
    tile = pl.program_id(1)
    tp = lax.axis_index("tp")
    for group in range(2):

        @pl.when(layer == 1 - group)
        def _():
            for lane in range(8):
                lane_bits = step_bits(tile, lane)
                spots = [place(lane_bits, color, tp) for color in range(COLORS)]
                for tensor in range(2):
                    for block in range(8):
                        color, slot = WHERE[group][tensor, block]
                        row, col = 64 * lane + 16 * (block // 2), 128 * (block % 2)
                        n_buf[tensor, row : row + 16, col : col + 128] = gat[group][color][slot, spots[color]]

    for cut in range(4):
        cols = slice(512 * cut, 512 * (cut + 1))
        change = dot(n_buf[0], q_out[0, cols, :], 1, 1)
        out_new[0, :, cols] = (w_out[0, :, cols].astype(F32) - STEP_SIZE * change).astype(BF16)
        change = dot(p_in[0, cols, :], n_buf[1], 1, 1)
        in_new[0, cols, :] = (w_in[0, cols, :].astype(F32) - STEP_SIZE * change).astype(BF16)


def local_step(x_rows, g_rows, w_in, w_out, p_in, q_out, m_in, v_in, m_out, v_out):
    def gathered(outs, ins):
        return jnp.stack([outs[1], ins[1].T, outs[0], ins[0].T])

    any_spec = pl.BlockSpec(memory_space=pl.ANY)
    vmem_spec = pl.BlockSpec(memory_space=pltpu.VMEM)
    shares = [jax.ShapeDtypeStruct((len(items), DP, 16, 128), BF16) for colors in BLOCKS for items in colors]
    moments = jax.ShapeDtypeStruct((4, 64, RANK), F32)
    results = pl.pallas_call(
        step_kernel,
        out_shape=shares + [moments, moments],
        in_specs=[any_spec] * 6 + [vmem_spec] * 2,
        out_specs=[any_spec] * 6 + [vmem_spec] * 2,
        scratch_shapes=[pltpu.VMEM(s.shape, F32) for s in shares]
        + [pltpu.VMEM((s.shape[0], DP - 1, 16, 128), F32) for s in shares]
        + [pltpu.VMEM(s.shape, BF16) for s in shares]
        + [
            pltpu.VMEM((TOK, D), BF16),
            pltpu.VMEM((TOK, D), BF16),
            pltpu.VMEM((TOK, F), BF16),
            pltpu.VMEM((TOK, F), BF16),
            pltpu.VMEM((TOK, F), BF16),
            pltpu.VMEM((SLOTS, 4, TILE, TILE), BF16),
            pltpu.VMEM((2, D, RANK), BF16),
            pltpu.VMEM((TOK, 3 * RANK), BF16),
            pltpu.VMEM((TOK, 3 * RANK), BF16),
            pltpu.VMEM((TOK, 3 * RANK), BF16),
            pltpu.VMEM((TOK, 3 * RANK), BF16),
            pltpu.SemaphoreType.DMA((SLOTS,)),
            pltpu.SemaphoreType.DMA((2,)),
            pltpu.SemaphoreType.DMA((2,)),
            pltpu.SemaphoreType.DMA((2, 3)),
            pltpu.SemaphoreType.DMA((2, 4)),
            pltpu.SemaphoreType.DMA((2, 4)),
            pltpu.SemaphoreType.DMA((2, 3, 20)),
            pltpu.SemaphoreType.DMA((2, 3, 20)),
        ],
        compiler_params=pltpu.CompilerParams(
            collective_id=0, has_side_effects=True, vmem_limit_bytes=67_000_000),
        name="galore_step",
    )(x_rows, g_rows, w_in, w_out, p_in, q_out, gathered(m_out, m_in), gathered(v_out, v_in))
    shares_new, (m_new, v_new) = results[:6], results[6:]

    layers = w_in.shape[0]
    in_block = pl.BlockSpec((1, D, TILE), lambda i, j: (layers - 1 - i, 0, j))
    out_block = pl.BlockSpec((1, TILE, D), lambda i, j: (layers - 1 - i, j, 0))
    basis = pl.BlockSpec((1, D, RANK), lambda i, j: (layers - 1 - i, 0, 0))
    w_in_new, w_out_new = pl.pallas_call(
        functools.partial(apply_kernel, layers),
        grid=(layers, F // TILE),
        out_shape=[jax.ShapeDtypeStruct(w_in.shape, BF16), jax.ShapeDtypeStruct(w_out.shape, BF16)],
        in_specs=[in_block, out_block, basis, basis] + [vmem_spec] * 6,
        out_specs=[in_block, out_block],
        scratch_shapes=[pltpu.VMEM((2, TILE, RANK), BF16)],
        compiler_params=pltpu.CompilerParams(vmem_limit_bytes=60_000_000),
        name="galore_apply",
    )(w_in, w_out, p_in, q_out, *shares_new)

    def split_moments(values):
        return jnp.stack([values[3].T, values[1].T]), jnp.stack([values[2], values[0]])

    m_in_new, m_out_new = split_moments(m_new)
    v_in_new, v_out_new = split_moments(v_new)
    return w_in_new, w_out_new, m_in_new, v_in_new, m_out_new, v_out_new


def solution(mesh):
    weight_in_spec = P(None, None, "tp")
    weight_out_spec = P(None, "tp", None)
    moment_in_spec = P(None, None, ("tp", "dp"))
    moment_out_spec = P(None, ("tp", "dp"), None)
    return jax.shard_map(
        local_step,
        mesh=mesh,
        in_specs=(P("dp", None), P("dp", None), weight_in_spec, weight_out_spec, P(), P(),
                  moment_in_spec, moment_in_spec, moment_out_spec, moment_out_spec),
        out_specs=(weight_in_spec, weight_out_spec, moment_in_spec, moment_in_spec, moment_out_spec, moment_out_spec),
        check_vma=False,
    )
```

```python
import functools

import jax
import jax.numpy as jnp
from jax import lax
from jax.experimental import pallas as pl
from jax.experimental.pallas import tpu as pltpu
from jax.sharding import PartitionSpec as P

BETA1 = 0.9
BETA2 = 0.999
EPSILON = 1e-8
STEP = 2
STEP_SIZE = 0.03 * 0.25
CORR_MOM = 1.0 - BETA1 ** STEP
CORR_VAR = 1.0 - BETA2 ** STEP

MESH = pl.DeviceIdType.MESH
BF16 = jnp.bfloat16
F32 = jnp.float32

TOK = 256
D = 2048
F = 4096
RANK = 256
DP = 64
TILE = 512
QUARTERS = range(4)
CHUNKS = 8
SLOTS = 4
DIMS = 6
COLORS = 3

CUTS = (((0, 3, 6, 8), (0, 2, 4, 8)), ((0, 3, 6, 8), (0, 3, 5, 8)))
BLOCKS = tuple(
    tuple(
        tuple((tensor, block) for tensor, cut in enumerate(cuts) for block in range(cut[color], cut[color + 1]))
        for color in range(COLORS)
    )
    for cuts in CUTS
)
WHERE = tuple(
    {item: (color, slot) for color, items in enumerate(colors) for slot, item in enumerate(items)} for colors in BLOCKS
)
FIRST_PART = tuple(CUTS[0][0][color + 1] - CUTS[0][0][color] for color in range(COLORS))


def ring_bits(position):
    high = lax.div(position, 2)
    return [lax.rem(high + position, 2), high]


def device_bits(dp):
    return ring_bits(lax.rem(dp, 4)) + ring_bits(lax.rem(lax.div(dp, 4), 4)) + ring_bits(lax.div(dp, 16))


def step_bits(tile, lane):
    x = lane % 4
    odd = lax.rem(tile, 2)
    y_low = odd if lane < 4 else 1 - odd
    z_high = lax.div(tile, 4)
    z_low = lax.rem(z_high + lax.rem(lax.div(tile, 2), 2), 2)
    return [(x // 2 + x) % 2, x // 2, y_low, odd, z_low, z_high]


def stage_dim(color, stage, core):
    return (2 * color + core + stage) % DIMS


def place(bits, color, tp):
    at = [sum(bits[stage_dim(color, stage, core)] * (32 >> stage) for stage in range(DIMS)) for core in range(2)]
    return at[0] * (1 - tp) + at[1] * tp


def flip(dp, dim):
    stride = 4 ** (dim // 2)
    position = lax.rem(lax.div(dp, stride), 4)
    other = 3 - position if dim % 2 else position + 1 - 2 * lax.rem(position, 2)
    return dp + (other - position) * stride


def by_core(tp, function, color, stage):
    zero, one = (function(stage_dim(color, stage, core)) for core in range(2))
    return zero * (1 - tp) + one * tp


def dot(left, right, left_dim=1, right_dim=0):
    return lax.dot_general(left, right, (((left_dim,), (right_dim,)), ((), ())), preferred_element_type=F32)


GELU_A = 0.7978845608028654
GELU_B = 0.044715


def gelu(z):
    return 0.5 * z * (1.0 + jnp.tanh(GELU_A * (z + GELU_B * z * z * z)))


def gelu_grad(z):
    square = z * z
    t = jnp.tanh(GELU_A * (z + GELU_B * z * square))
    return 0.5 * (1.0 + t) + 0.5 * z * (1.0 - t * t) * (GELU_A * (1.0 + 3.0 * GELU_B * square))


def step_kernel(x_hbm, g_hbm, w_in, w_out, p_in, q_out, m_in, v_in, m_out, v_out, *rest):
    rest = iter(rest)

    def by_group():
        return tuple(tuple(next(rest) for color in range(COLORS)) for group in range(2))

    n_out = by_group()
    m_new, v_new = next(rest), next(rest)
    red, got, gat = by_group(), by_group(), by_group()
    (h_buf, g_buf, a_buf, z0_buf, z1_buf, w_buf, pq_buf, hp0, gq1, hp1, gq0,
     w_sem, in_sem, pq_sem, out_sem, pair_send, pair_recv, send_sem, recv_sem) = rest
    dp = lax.axis_index("dp")
    tp = lax.axis_index("tp")
    bits = device_bits(dp)

    def direct_device(color, mask):
        ends = []
        for core in range(2):
            end = dp
            for stage in range(3, DIMS):
                if mask & (32 >> stage):
                    end = flip(end, stage_dim(color, stage, core))
            ends.append(end)
        return ends[0] * (1 - tp) + ends[1] * tp

    barrier = pltpu.get_barrier_semaphore()
    greeted = set()
    for color in range(COLORS):
        for mask in range(1, 8):
            dims = tuple(
                tuple(sorted(stage_dim(color, stage, core) for stage in range(3, DIMS) if mask & (32 >> stage)))
                for core in range(2))
            if dims not in greeted:
                greeted.add(dims)
                pl.semaphore_signal(barrier, device_id={"dp": direct_device(color, mask)}, device_id_type=MESH)
    pl.semaphore_signal(barrier, device_id={"tp": 1 - tp}, device_id_type=MESH)
    pl.semaphore_wait(barrier, len(greeted) + 1)

    def block_of(phase, chunk, q):
        name, layer = phase
        half, rest_ = lax.rem(chunk, 2), lax.div(chunk, 2)
        if name == "z":
            return w_in.at[layer, pl.ds(TILE * q, TILE), pl.ds(pl.multiple_of(TILE * chunk, TILE), TILE)]
        if name == "h":
            return w_out.at[layer, pl.ds(pl.multiple_of(2048 * half, TILE) + TILE * q, TILE),
                            pl.ds(pl.multiple_of(TILE * rest_, TILE), TILE)]
        if name == "da":
            return w_out.at[layer, pl.ds(pl.multiple_of(TILE * chunk, TILE), TILE), pl.ds(TILE * q, TILE)]
        return w_in.at[layer, pl.ds(pl.multiple_of(TILE * rest_, TILE), TILE),
                       pl.ds(pl.multiple_of(2048 * half + TILE * q, TILE), TILE)]

    def start_chunk(phase, chunk):
        slot = lax.rem(chunk, SLOTS)
        for q in QUARTERS:
            pltpu.make_async_copy(block_of(phase, chunk, q), w_buf.at[slot, q], w_sem.at[slot]).start()

    def wait_chunk(chunk):
        slot = lax.rem(chunk, SLOTS)
        pltpu.make_async_copy(w_buf.at[slot], w_buf.at[slot], w_sem.at[slot]).wait()
        return slot

    phases = (("z", 0), ("h", 0), ("z", 1), ("da", 1), ("b", 1), ("da", 0))

    def take_chunk(index, chunk):
        ahead = chunk + SLOTS - 1

        @pl.when(ahead < CHUNKS)
        def _():
            start_chunk(phases[index], ahead)

        if index + 1 < len(phases):

            @pl.when(ahead >= CHUNKS)
            def _():
                start_chunk(phases[index + 1], ahead - CHUNKS)

        return wait_chunk(chunk)

    def load_pq(ref, layer, slot):
        pltpu.make_async_copy(ref.at[layer], pq_buf.at[slot], pq_sem.at[slot]).start()

    def wait_pq(ref, slot):
        pltpu.make_async_copy(ref.at[0], pq_buf.at[slot], pq_sem.at[slot]).wait()

    x_copy = pltpu.make_async_copy(x_hbm, h_buf, in_sem.at[0])
    g_copy = pltpu.make_async_copy(g_hbm, g_buf, in_sem.at[1])
    x_copy.start()
    for chunk in range(SLOTS - 1):
        start_chunk(phases[0], jnp.int32(chunk))
    g_copy.start()
    load_pq(p_in, 0, 0)
    load_pq(q_out, 1, 1)

    def split(values, out_ref):
        for part in range(3):
            piece = values.astype(BF16)
            out_ref[:, RANK * part : RANK * (part + 1)] = piece
            values = values - piece.astype(F32)

    def project(rows, parts, group, tensor, tile):
        wide = dot(rows, parts[...], 0, 0)
        total = wide[:, 2 * RANK : 3 * RANK] + wide[:, RANK : 2 * RANK] + wide[:, 0:RANK]
        for lane in range(8):
            lane_bits = step_bits(tile, lane)
            spots = [place(lane_bits, color, tp) for color in range(COLORS)]
            for block in range(8):
                color, slot = WHERE[group][tensor, block]
                row, col = 64 * lane + 16 * (block // 2), 128 * (block % 2)
                red[group][color][slot, spots[color]] = total[row : row + 16, col : col + 128]

    def columns(tile):
        return pl.ds(pl.multiple_of(TILE * tile, TILE), TILE)

    def pair_copy(exchange, n):
        return pltpu.make_async_remote_copy(
            src_ref=red[1][0].at[n], dst_ref=red[1][1 + exchange].at[n],
            send_sem=pair_send.at[exchange, n], recv_sem=pair_recv.at[exchange, n],
            device_id={"tp": 1 - tp}, device_id_type=MESH)

    def pair_send_tile(exchange, n, values):
        for a in range(16):
            for b in QUARTERS:
                red[1][0][n, 4 * a + b] = values[16 * a : 16 * a + 16, 128 * b : 128 * b + 128]
        pair_copy(exchange, n).start()

    def pair_add(exchange, state):
        def one(n, carry):
            pair_copy(exchange, n).wait()
            for a in range(16):
                for b in QUARTERS:
                    cols = pl.ds(pl.multiple_of(TILE * n + 128 * b, 128), 128)
                    both = red[1][0][n, 4 * a + b] + red[1][1 + exchange][n, 4 * a + b]
                    state[16 * a : 16 * a + 16, cols] = (
                        state[16 * a : 16 * a + 16, cols].astype(F32) + both).astype(BF16)
            return carry

        lax.fori_loop(0, 4, one, 0)

    own = [place(bits, color, tp) for color in range(COLORS)]

    def message(group, color, number, source, target, device):
        return pltpu.make_async_remote_copy(
            src_ref=source, dst_ref=target,
            send_sem=send_sem.at[group, color, number], recv_sem=recv_sem.at[group, color, number],
            device_id={"dp": device}, device_id_type=MESH)

    def start_of(color, stage):
        width = DP >> stage
        return lax.div(own[color], width) * width

    def bit(color, stage):
        return lax.rem(lax.div(own[color], 32 >> stage), 2)

    def cut(group, color, stage, part):
        half = 32 >> stage
        every = slice(0, len(BLOCKS[group][color]))
        if stage == 2:
            return every, 0, 0, half
        if group == 0 and stage == 0:
            first = FIRST_PART[color]
            return (slice(first, every.stop) if part else slice(0, first)), 0, 0, half
        ahead = bit(color, stage + 1)
        quarter = half // 2
        return every, (ahead if part else 1 - ahead) * quarter, part * quarter, quarter

    def reduce_copy(group, color, stage, part):
        slots, offset, into, size = cut(group, color, stage, part)
        source = start_of(color, stage) + (1 - bit(color, stage)) * (32 >> stage) + offset
        target = DP - (DP >> stage) + into
        return message(group, color, 2 * stage + part, red[group][color].at[slots, pl.ds(source, size)],
                       got[group][color].at[slots, pl.ds(target, size)],
                       by_core(tp, functools.partial(flip, dp), color, stage))

    def reduce_send(group, color, stage, part):
        reduce_copy(group, color, stage, part).start()

    def reduce_add(group, color, stage, part):
        reduce_copy(group, color, stage, part).wait()
        slots, offset, into, size = cut(group, color, stage, part)
        kept = start_of(color, stage + 1) + offset
        target = DP - (DP >> stage) + into
        step = 4

        def one(i, carry):
            for slot in range(slots.start, slots.stop):
                to = pl.ds(kept + step * i, step)
                red[group][color][slot, to] = (
                    red[group][color][slot, to] + got[group][color][slot, pl.ds(target + step * i, step)])
            return carry

        lax.fori_loop(0, size // step, one, 0)

    def direct_share(color, mask):
        share = own[color]
        for stage in range(3, DIMS):
            weight = 32 >> stage
            if mask & weight:
                share = share + weight * (1 - 2 * bit(color, stage))
        return share

    def direct_reduce(group, color, mask):
        return message(group, color, 4 + mask, red[group][color].at[:, pl.ds(direct_share(color, mask), 1)],
                       got[group][color].at[:, pl.ds(55 + mask, 1)], direct_device(color, mask))

    def direct_gather(group, color, mask):
        spot = gat[group][color].at[:, pl.ds(own[color], 1)]
        return message(group, color, 11 + mask, spot, spot, direct_device(color, mask))

    def update(group, color):
        for slot, (tensor, block) in enumerate(BLOCKS[group][color]):
            row, col = 16 * (block // 2), 128 * (block % 2)
            spot = (2 * group + tensor, slice(row, row + 16), slice(col, col + 128))
            layer = 1 - group
            old = (layer, *spot[1:])
            old_m, old_v = (m_in[old], v_in[old]) if tensor else (m_out[old], v_out[old])
            grad = red[group][color][slot, own[color]]
            for mask in range(1, 8):
                grad = grad + got[group][color][slot, 55 + mask]
            moment = BETA1 * old_m + (1.0 - BETA1) * grad
            second = BETA2 * old_v + (1.0 - BETA2) * grad * grad
            m_new[spot] = moment
            v_new[spot] = second
            direction = (moment / CORR_MOM) / (jnp.sqrt(second / CORR_VAR) + EPSILON)
            gat[group][color][slot, own[color]] = direction.astype(BF16)

    def eight(color, near, far):
        return start_of(color, 3) + near * 8 * (1 - 2 * bit(color, 2)) + far * 16 * (1 - 2 * bit(color, 1))

    def gather_copy(group, color, stage, near, far):
        spot = gat[group][color].at[:, pl.ds(eight(color, near, far), 8)]
        return message(group, color, 19 + (near if stage == 1 else 2 + near + 2 * far if stage == 0 else 6), spot, spot,
                       by_core(tp, functools.partial(flip, dp), color, stage))

    def gather_start(group, color):
        for stage in (2, 1, 0):
            gather_copy(group, color, stage, 0, 0).start()

    def gather_near(group, color):
        gather_copy(group, color, 2, 0, 0).wait()
        for stage in (1, 0):
            gather_copy(group, color, stage, 1, 0).start()

    def gather_far(group, color):
        for near in range(2):
            gather_copy(group, color, 1, near, 0).wait()
            gather_copy(group, color, 0, near, 1).start()

    def gather_end(group, color):
        for far in range(2):
            for near in range(2):
                gather_copy(group, color, 0, near, far).wait()

    def write_out(group, color):
        return pltpu.make_async_copy(gat[group][color], n_out[group][color], out_sem.at[group, color])

    def colors(function, *args):
        for color in range(COLORS):
            function(*args[:1], color, *args[1:])

    def take(group, color, stage, part, then):
        reduce_add(group, color, stage, part)
        for number in range(then):
            reduce_send(group, color, stage + 1, number)

    def direct_start(group, color):
        for mask in range(1, 8):
            direct_reduce(group, color, mask).start()

    def direct_end(group, color):
        for mask in range(1, 8):
            direct_reduce(group, color, mask).wait()
        update(group, color)
        for mask in range(1, 8):
            direct_gather(group, color, mask).start()

    def direct_gathered(group, color):
        for mask in range(1, 8):
            direct_gather(group, color, mask).wait()
        gather_start(group, color)

    def last_stage(group, color):
        reduce_add(group, color, 2, 0)
        direct_start(group, color)

    def finish(group, color):
        gather_end(group, color)
        write_out(group, color).start()

    def forward(slot):
        return sum(dot(h_buf[:, TILE * q : TILE * (q + 1)], w_buf[slot, q]) for q in QUARTERS).astype(BF16)

    def backward(slot):
        return sum(dot(g_buf[:, TILE * q : TILE * (q + 1)], w_buf[slot, q], 1, 1) for q in QUARTERS)

    x_copy.wait()

    def z0_step(tile, carry):
        slot = take_chunk(0, tile)
        z = forward(slot)
        z0_buf[:, columns(tile)] = z
        a_buf[:, columns(tile)] = gelu(z.astype(F32)).astype(BF16)
        return carry

    lax.fori_loop(0, CHUNKS, z0_step, 0)

    def h_step(n, carry):
        total = None
        for half in range(2):
            slot = take_chunk(1, 2 * n + half)
            for q in QUARTERS:
                at = 2048 * half + TILE * q
                term = dot(a_buf[:, at : at + TILE], w_buf[slot, q])
                total = term if total is None else total + term
        pair_send_tile(0, n, total)
        return carry

    lax.fori_loop(0, 4, h_step, 0)
    wait_pq(p_in, 0)
    split(dot(h_buf[...], pq_buf[0]), hp0)
    load_pq(p_in, 1, 0)
    g_copy.wait()
    wait_pq(q_out, 1)
    split(dot(g_buf[...], pq_buf[1]), gq1)
    load_pq(q_out, 0, 1)
    pair_add(0, h_buf)

    def z1_step(tile, carry):
        slot = take_chunk(2, tile)
        z = forward(slot)
        z1_buf[:, columns(tile)] = z
        project(gelu(z.astype(F32)).astype(BF16), gq1, 0, 0, tile)
        return carry

    lax.fori_loop(0, CHUNKS, z1_step, 0)
    colors(reduce_send, 0, 0, 0)
    wait_pq(p_in, 0)
    split(dot(h_buf[...], pq_buf[0]), hp1)

    def da1_step(tile, carry):
        slot = take_chunk(3, tile)
        d_act = backward(slot)
        dz = (gelu_grad(z1_buf[:, columns(tile)].astype(F32)) * d_act).astype(BF16)
        z1_buf[:, columns(tile)] = dz
        project(dz, hp1, 0, 1, tile)
        return carry

    lax.fori_loop(0, CHUNKS, da1_step, 0)
    colors(reduce_send, 0, 0, 1)

    def b_step(n, carry):
        total = None
        for half in range(2):
            slot = take_chunk(4, 2 * n + half)
            for q in QUARTERS:
                at = 2048 * half + TILE * q
                term = dot(z1_buf[:, at : at + TILE], w_buf[slot, q], 1, 1)
                total = term if total is None else total + term
        pair_send_tile(1, n, total)
        return carry

    lax.fori_loop(0, 4, b_step, 0)
    wait_pq(q_out, 1)
    pair_add(1, g_buf)
    split(dot(g_buf[...], pq_buf[1]), gq0)

    def da0_step(tile, carry):
        slot = take_chunk(5, tile)

        @pl.when(tile == 1)
        def _():
            colors(take, 0, 0, 0, 0)
            colors(take, 0, 0, 1, 2)

        project(a_buf[:, columns(tile)], gq0, 1, 0, tile)
        d_act = backward(slot)
        dz = (gelu_grad(z0_buf[:, columns(tile)].astype(F32)) * d_act).astype(BF16)
        project(dz, hp0, 1, 1, tile)
        return carry

    lax.fori_loop(0, CHUNKS, da0_step, 0)

    colors(reduce_send, 1, 0, 0)
    colors(take, 0, 1, 0, 1)
    colors(reduce_send, 1, 0, 1)
    colors(take, 0, 1, 1, 0)
    colors(take, 1, 0, 0, 2)
    colors(last_stage, 0)
    colors(take, 1, 0, 1, 0)
    colors(take, 1, 1, 0, 1)
    colors(direct_end, 0)
    colors(take, 1, 1, 1, 0)
    colors(direct_gathered, 0)
    colors(last_stage, 1)
    colors(gather_near, 0)
    colors(direct_end, 1)
    colors(gather_far, 0)
    colors(direct_gathered, 1)
    colors(finish, 0)
    colors(gather_near, 1)
    colors(gather_far, 1)
    colors(finish, 1)
    for group in range(2):
        for color in range(COLORS):
            write_out(group, color).wait()


READS = 3
WRITES = 2


def apply_kernel(w_in, w_out, p_in, q_out, m_step, v_step, *rest):
    rest = iter(rest)
    shares = [next(rest) for item in range(6)]
    in_new, out_new, m_in, v_in, m_out, v_out = (next(rest) for item in range(6))
    gat = [next(rest) for item in range(6)]
    (p_buf, q_buf, in_read, out_read, in_write, out_write, n_buf,
     share_sem, basis_sem, read_sem, write_sem) = rest
    tp = lax.axis_index("tp")
    pairs = 2 * CHUNKS

    def tile_of(ref, pair, rows):
        layer = 1 - lax.div(pair, CHUNKS)
        at = pl.ds(pl.multiple_of(TILE * lax.rem(pair, CHUNKS), TILE), TILE)
        return ref.at[layer, at] if rows else ref.at[layer, :, at]

    def read(pair, rows):
        ref, buf = (w_out, out_read) if rows else (w_in, in_read)
        slot = lax.rem(pair, READS)
        return pltpu.make_async_copy(tile_of(ref, pair, rows), buf.at[slot], read_sem.at[rows, slot])

    def write(pair, rows):
        ref, buf = (out_new, out_write) if rows else (in_new, in_write)
        slot = lax.rem(pair, WRITES)
        return pltpu.make_async_copy(buf.at[slot], tile_of(ref, pair, rows), write_sem.at[rows, slot])

    def share_copy(item):
        return pltpu.make_async_copy(shares[item], gat[item], share_sem.at[item])

    def basis_copy(layer, rows):
        ref, buf = (q_out, q_buf) if rows else (p_in, p_buf)
        return pltpu.make_async_copy(ref.at[layer], buf.at[layer], basis_sem.at[layer, rows])

    for group in range(2):
        for color in range(COLORS):
            share_copy(COLORS * group + color).start()
        for rows in (1, 0):
            basis_copy(1 - group, rows).start()
        for pair in range(1 if group == 0 else READS):
            if group == 0 or pair:
                for rows in (1, 0):
                    read(jnp.int32(pair), rows).start()

    for step, in_ref, out_ref in ((m_step, m_in, m_out), (v_step, v_in, v_out)):
        for layer in range(2):
            out_ref[layer] = step[2 - 2 * layer]
            in_ref[layer] = step[3 - 2 * layer]

    def gather(group, tile):
        for lane in range(8):
            lane_bits = step_bits(tile, lane)
            spots = [place(lane_bits, color, tp) for color in range(COLORS)]
            for tensor in range(2):
                for block in range(8):
                    color, slot = WHERE[group][tensor, block]
                    row, col = 64 * lane + 16 * (block // 2), 128 * (block % 2)
                    n_buf[tensor, row : row + 16, col : col + 128] = gat[COLORS * group + color][slot, spots[color]]

    def one(pair, carry):
        layer = 1 - lax.div(pair, CHUNKS)
        for group in range(2):

            @pl.when(pair == CHUNKS * group)
            def _():
                for color in range(COLORS):
                    share_copy(COLORS * group + color).wait()
                for rows in (1, 0):
                    basis_copy(1 - group, rows).wait()

            @pl.when(layer == 1 - group)
            def _():
                gather(group, lax.rem(pair, CHUNKS))

        for rows in (1, 0):
            source, target = (out_read, out_write) if rows else (in_read, in_write)
            read(pair, rows).wait()

            @pl.when(pair >= WRITES)
            def _():
                write(pair - WRITES, rows).wait()

            slot, to = lax.rem(pair, READS), lax.rem(pair, WRITES)
            for cut in QUARTERS:
                at = slice(TILE * cut, TILE * (cut + 1))
                if rows:
                    spot = (slice(None), at)
                    change = dot(n_buf[0], q_buf[layer, at, :], 1, 1)
                else:
                    spot = (at, slice(None))
                    change = dot(p_buf[layer, at, :], n_buf[1], 1, 1)
                target[(to, *spot)] = (source[(slot, *spot)].astype(F32) - STEP_SIZE * change).astype(BF16)
            write(pair, rows).start()

            @pl.when(pair + READS < pairs)
            def _():
                read(pair + READS, rows).start()

        return carry

    lax.fori_loop(0, pairs, one, 0)
    for back in range(WRITES):
        for rows in (1, 0):
            write(jnp.int32(pairs - WRITES + back), rows).wait()


def local_step(x_rows, g_rows, w_in, w_out, p_in, q_out, m_in, v_in, m_out, v_out):
    m_in, v_in = (jnp.swapaxes(moment, 1, 2) for moment in (m_in, v_in))
    any_spec = pl.BlockSpec(memory_space=pl.ANY)
    vmem_spec = pl.BlockSpec(memory_space=pltpu.VMEM)
    shares = [jax.ShapeDtypeStruct((len(items), DP, 16, 128), BF16) for colors in BLOCKS for items in colors]
    moments = jax.ShapeDtypeStruct((4, 64, RANK), F32)
    rows_buf, wide_buf = pltpu.VMEM((TOK, D), BF16), pltpu.VMEM((TOK, F), BF16)
    parts_buf = pltpu.VMEM((TOK, 3 * RANK), BF16)
    basis_buf = pltpu.VMEM((2, D, RANK), BF16)
    dma = pltpu.SemaphoreType.DMA
    results = pl.pallas_call(
        step_kernel,
        out_shape=shares + [moments, moments],
        in_specs=[any_spec] * 6 + [vmem_spec] * 4,
        out_specs=[any_spec] * 6 + [vmem_spec] * 2,
        scratch_shapes=[pltpu.VMEM(s.shape, F32) for s in shares]
        + [pltpu.VMEM((s.shape[0], DP - 1, 16, 128), F32) for s in shares]
        + [pltpu.VMEM(s.shape, BF16) for s in shares]
        + [rows_buf] * 2
        + [wide_buf] * 3
        + [pltpu.VMEM((SLOTS, 4, TILE, TILE), BF16), basis_buf]
        + [parts_buf] * 4
        + [dma((SLOTS,)), dma((2,)), dma((2,)), dma((2, 3)), dma((2, 4)), dma((2, 4)), dma((2, 3, 26)), dma((2, 3, 26))],
        compiler_params=pltpu.CompilerParams(
            collective_id=0, has_side_effects=True, vmem_limit_bytes=67_000_000),
        name="galore_step",
    )(x_rows, g_rows, w_in, w_out, p_in, q_out, m_in, v_in, m_out, v_out)
    in_tile, out_tile = (D, TILE), (TILE, D)
    w_in_new, w_out_new, m_in, v_in, m_out, v_out = pl.pallas_call(
        apply_kernel,
        out_shape=[jax.ShapeDtypeStruct(w.shape, w.dtype) for w in (w_in, w_out, m_in, v_in, m_out, v_out)],
        in_specs=[any_spec] * 4 + [vmem_spec] * 2 + [any_spec] * 6,
        out_specs=[any_spec] * 2 + [vmem_spec] * 4,
        scratch_shapes=[pltpu.VMEM(s.shape, BF16) for s in shares]
        + [basis_buf] * 2
        + [pltpu.VMEM((READS, *in_tile), BF16), pltpu.VMEM((READS, *out_tile), BF16)]
        + [pltpu.VMEM((WRITES, *in_tile), BF16), pltpu.VMEM((WRITES, *out_tile), BF16)]
        + [pltpu.VMEM((2, TILE, RANK), BF16), dma((6,)), dma((2, 2)), dma((2, READS)), dma((2, WRITES))],
        compiler_params=pltpu.CompilerParams(vmem_limit_bytes=60_000_000),
        name="galore_apply",
    )(w_in, w_out, p_in, q_out, *results[6:], *results[:6])
    m_in, v_in = (jnp.swapaxes(moment, 1, 2) for moment in (m_in, v_in))
    return w_in_new, w_out_new, m_in, v_in, m_out, v_out


def solution(mesh):
    weight_in_spec = P(None, None, "tp")
    weight_out_spec = P(None, "tp", None)
    moment_in_spec = P(None, None, ("tp", "dp"))
    moment_out_spec = P(None, ("tp", "dp"), None)
    return jax.shard_map(
        local_step,
        mesh=mesh,
        in_specs=(P("dp", None), P("dp", None), weight_in_spec, weight_out_spec, P(), P(),
                  moment_in_spec, moment_in_spec, moment_out_spec, moment_out_spec),
        out_specs=(weight_in_spec, weight_out_spec, moment_in_spec, moment_in_spec, moment_out_spec, moment_out_spec),
        check_vma=False,
    )
```

```python
import functools

import jax
import jax.numpy as jnp
from jax import lax
from jax.experimental import pallas as pl
from jax.experimental.pallas import tpu as pltpu
from jax.sharding import PartitionSpec as P

BETA1 = 0.9
BETA2 = 0.999
EPSILON = 1e-8
STEP = 2
STEP_SIZE = 0.03 * 0.25
CORR_MOM = 1.0 - BETA1 ** STEP
CORR_VAR = 1.0 - BETA2 ** STEP

MESH = pl.DeviceIdType.MESH
BF16 = jnp.bfloat16
F32 = jnp.float32

TOK = 256
D = 2048
F = 4096
RANK = 256
DP = 64
TILE = 512
QUARTERS = range(4)
CHUNKS = 8
SLOTS = 4
DIMS = 6
COLORS = 3

CUTS = (((0, 3, 6, 8), (0, 2, 4, 8)), ((0, 3, 6, 8), (0, 3, 5, 8)))
BLOCKS = tuple(
    tuple(
        tuple((tensor, block) for tensor, cut in enumerate(cuts) for block in range(cut[color], cut[color + 1]))
        for color in range(COLORS)
    )
    for cuts in CUTS
)
WHERE = tuple(
    {item: (color, slot) for color, items in enumerate(colors) for slot, item in enumerate(items)} for colors in BLOCKS
)
FIRST_PART = tuple(CUTS[0][0][color + 1] - CUTS[0][0][color] for color in range(COLORS))


def ring_bits(position):
    high = lax.div(position, 2)
    return [lax.rem(high + position, 2), high]


def device_bits(dp):
    return ring_bits(lax.rem(dp, 4)) + ring_bits(lax.rem(lax.div(dp, 4), 4)) + ring_bits(lax.div(dp, 16))


def step_bits(tile, lane):
    x = lane % 4
    odd = lax.rem(tile, 2)
    y_low = odd if lane < 4 else 1 - odd
    z_high = lax.div(tile, 4)
    z_low = lax.rem(z_high + lax.rem(lax.div(tile, 2), 2), 2)
    return [(x // 2 + x) % 2, x // 2, y_low, odd, z_low, z_high]


def stage_dim(color, stage, core):
    return (2 * color + core + stage) % DIMS


def place(bits, color, tp):
    at = [sum(bits[stage_dim(color, stage, core)] * (32 >> stage) for stage in range(DIMS)) for core in range(2)]
    return at[0] * (1 - tp) + at[1] * tp


def flip(dp, dim):
    stride = 4 ** (dim // 2)
    position = lax.rem(lax.div(dp, stride), 4)
    other = 3 - position if dim % 2 else position + 1 - 2 * lax.rem(position, 2)
    return dp + (other - position) * stride


def by_core(tp, function, color, stage):
    zero, one = (function(stage_dim(color, stage, core)) for core in range(2))
    return zero * (1 - tp) + one * tp


def dot(left, right, left_dim=1, right_dim=0):
    return lax.dot_general(left, right, (((left_dim,), (right_dim,)), ((), ())), preferred_element_type=F32)


GELU_A = 0.7978845608028654
GELU_B = 0.044715


def gelu(z):
    return 0.5 * z * (1.0 + jnp.tanh(GELU_A * (z + GELU_B * z * z * z)))


def gelu_grad(z):
    square = z * z
    t = jnp.tanh(GELU_A * (z + GELU_B * z * square))
    return 0.5 * (1.0 + t) + 0.5 * z * (1.0 - t * t) * (GELU_A * (1.0 + 3.0 * GELU_B * square))


def step_kernel(x_hbm, g_hbm, w_in, w_out, p_in, q_out, m_in, v_in, m_out, v_out, *rest):
    rest = iter(rest)

    def by_group():
        return tuple(tuple(next(rest) for color in range(COLORS)) for group in range(2))

    n_out = by_group()
    m_new, v_new = next(rest), next(rest)
    red, got, gat = by_group(), by_group(), by_group()
    (h_buf, g_buf, a_buf, z0_buf, z1_buf, w_buf, pq_buf, hp0, gq1, hp1, gq0,
     w_sem, in_sem, pq_sem, out_sem, pair_send, pair_recv, send_sem, recv_sem) = rest
    dp = lax.axis_index("dp")
    tp = lax.axis_index("tp")
    bits = device_bits(dp)

    def direct_device(color, mask):
        ends = []
        for core in range(2):
            end = dp
            for stage in range(3, DIMS):
                if mask & (32 >> stage):
                    end = flip(end, stage_dim(color, stage, core))
            ends.append(end)
        return ends[0] * (1 - tp) + ends[1] * tp

    def block_of(phase, chunk, q):
        name, layer = phase
        half, rest_ = lax.rem(chunk, 2), lax.div(chunk, 2)
        if name == "z":
            return w_in.at[layer, pl.ds(TILE * q, TILE), pl.ds(pl.multiple_of(TILE * chunk, TILE), TILE)]
        if name == "h":
            return w_out.at[layer, pl.ds(pl.multiple_of(2048 * half, TILE) + TILE * q, TILE),
                            pl.ds(pl.multiple_of(TILE * rest_, TILE), TILE)]
        if name == "da":
            return w_out.at[layer, pl.ds(pl.multiple_of(TILE * chunk, TILE), TILE), pl.ds(TILE * q, TILE)]
        return w_in.at[layer, pl.ds(pl.multiple_of(TILE * rest_, TILE), TILE),
                       pl.ds(pl.multiple_of(2048 * half + TILE * q, TILE), TILE)]

    def start_chunk(phase, chunk):
        slot = lax.rem(chunk, SLOTS)
        for q in QUARTERS:
            pltpu.make_async_copy(block_of(phase, chunk, q), w_buf.at[slot, q], w_sem.at[slot]).start()

    def wait_chunk(chunk):
        slot = lax.rem(chunk, SLOTS)
        pltpu.make_async_copy(w_buf.at[slot], w_buf.at[slot], w_sem.at[slot]).wait()
        return slot

    phases = (("z", 0), ("h", 0), ("z", 1), ("da", 1), ("b", 1), ("da", 0))

    def take_chunk(index, chunk):
        ahead = chunk + SLOTS - 1

        @pl.when(ahead < CHUNKS)
        def _():
            start_chunk(phases[index], ahead)

        if index + 1 < len(phases):

            @pl.when(ahead >= CHUNKS)
            def _():
                start_chunk(phases[index + 1], ahead - CHUNKS)

        return wait_chunk(chunk)

    def load_pq(ref, layer, slot):
        pltpu.make_async_copy(ref.at[layer], pq_buf.at[slot], pq_sem.at[slot]).start()

    def wait_pq(ref, slot):
        pltpu.make_async_copy(ref.at[0], pq_buf.at[slot], pq_sem.at[slot]).wait()

    x_copy = pltpu.make_async_copy(x_hbm, h_buf, in_sem.at[0])
    g_copy = pltpu.make_async_copy(g_hbm, g_buf, in_sem.at[1])
    x_copy.start()
    for chunk in range(SLOTS - 1):
        start_chunk(phases[0], jnp.int32(chunk))
    g_copy.start()
    load_pq(p_in, 0, 0)
    load_pq(q_out, 1, 1)

    barrier = pltpu.get_barrier_semaphore()
    greeted = set()
    for color in range(COLORS):
        for mask in range(1, 8):
            dims = tuple(
                tuple(sorted(stage_dim(color, stage, core) for stage in range(3, DIMS) if mask & (32 >> stage)))
                for core in range(2))
            if dims not in greeted:
                greeted.add(dims)
                pl.semaphore_signal(barrier, device_id={"dp": direct_device(color, mask)}, device_id_type=MESH)
    pl.semaphore_signal(barrier, device_id={"tp": 1 - tp}, device_id_type=MESH)

    def split(values, out_ref):
        for part in range(3):
            piece = values.astype(BF16)
            out_ref[:, RANK * part : RANK * (part + 1)] = piece
            values = values - piece.astype(F32)

    def project(rows, parts, group, tensor, tile):
        wide = dot(rows, parts[...], 0, 0)
        total = wide[:, 2 * RANK : 3 * RANK] + wide[:, RANK : 2 * RANK] + wide[:, 0:RANK]
        for lane in range(8):
            lane_bits = step_bits(tile, lane)
            spots = [place(lane_bits, color, tp) for color in range(COLORS)]
            for block in range(8):
                color, slot = WHERE[group][tensor, block]
                row, col = 64 * lane + 16 * (block // 2), 128 * (block % 2)
                red[group][color][slot, spots[color]] = total[row : row + 16, col : col + 128]

    def columns(tile):
        return pl.ds(pl.multiple_of(TILE * tile, TILE), TILE)

    def pair_copy(exchange, n):
        return pltpu.make_async_remote_copy(
            src_ref=red[1][0].at[n], dst_ref=red[1][1 + exchange].at[n],
            send_sem=pair_send.at[exchange, n], recv_sem=pair_recv.at[exchange, n],
            device_id={"tp": 1 - tp}, device_id_type=MESH)

    def pair_send_tile(exchange, n, values):
        for a in range(16):
            for b in QUARTERS:
                red[1][0][n, 4 * a + b] = values[16 * a : 16 * a + 16, 128 * b : 128 * b + 128]
        pair_copy(exchange, n).start()

    def pair_add(exchange, state):
        def one(n, carry):
            pair_copy(exchange, n).wait()
            for a in range(16):
                for b in QUARTERS:
                    cols = pl.ds(pl.multiple_of(TILE * n + 128 * b, 128), 128)
                    both = red[1][0][n, 4 * a + b] + red[1][1 + exchange][n, 4 * a + b]
                    state[16 * a : 16 * a + 16, cols] = (
                        state[16 * a : 16 * a + 16, cols].astype(F32) + both).astype(BF16)
            return carry

        lax.fori_loop(0, 4, one, 0)

    own = [place(bits, color, tp) for color in range(COLORS)]

    def message(group, color, number, source, target, device):
        return pltpu.make_async_remote_copy(
            src_ref=source, dst_ref=target,
            send_sem=send_sem.at[group, color, number], recv_sem=recv_sem.at[group, color, number],
            device_id={"dp": device}, device_id_type=MESH)

    def start_of(color, stage):
        width = DP >> stage
        return lax.div(own[color], width) * width

    def bit(color, stage):
        return lax.rem(lax.div(own[color], 32 >> stage), 2)

    def cut(group, color, stage, part):
        half = 32 >> stage
        every = slice(0, len(BLOCKS[group][color]))
        if stage == 2:
            return every, 0, 0, half
        if stage == 0:
            first = FIRST_PART[color]
            every = slice(first, every.stop) if part >= 2 else slice(0, first)
            part = part % 2
        ahead = bit(color, stage + 1)
        quarter = half // 2
        return every, (ahead if part else 1 - ahead) * quarter, part * quarter, quarter

    def reduce_copy(group, color, stage, part):
        slots, offset, into, size = cut(group, color, stage, part)
        source = start_of(color, stage) + (1 - bit(color, stage)) * (32 >> stage) + offset
        target = DP - (DP >> stage) + into
        return message(group, color, part + 2 * stage + (2 if stage else 0), red[group][color].at[slots, pl.ds(source, size)],
                       got[group][color].at[slots, pl.ds(target, size)],
                       by_core(tp, functools.partial(flip, dp), color, stage))

    def reduce_send(group, color, stage, part):
        reduce_copy(group, color, stage, part).start()

    def reduce_add(group, color, stage, part):
        reduce_copy(group, color, stage, part).wait()
        slots, offset, into, size = cut(group, color, stage, part)
        kept = start_of(color, stage + 1) + offset
        target = DP - (DP >> stage) + into
        step = 4

        def one(i, carry):
            for slot in range(slots.start, slots.stop):
                to = pl.ds(kept + step * i, step)
                red[group][color][slot, to] = (
                    red[group][color][slot, to] + got[group][color][slot, pl.ds(target + step * i, step)])
            return carry

        lax.fori_loop(0, size // step, one, 0)

    def direct_share(color, mask):
        share = own[color]
        for stage in range(3, DIMS):
            weight = 32 >> stage
            if mask & weight:
                share = share + weight * (1 - 2 * bit(color, stage))
        return share

    def direct_reduce(group, color, mask):
        return message(group, color, 6 + mask, red[group][color].at[:, pl.ds(direct_share(color, mask), 1)],
                       got[group][color].at[:, pl.ds(55 + mask, 1)], direct_device(color, mask))

    def direct_gather(group, color, mask):
        spot = gat[group][color].at[:, pl.ds(own[color], 1)]
        return message(group, color, 13 + mask, spot, spot, direct_device(color, mask))

    def update(group, color):
        for slot, (tensor, block) in enumerate(BLOCKS[group][color]):
            row, col = 16 * (block // 2), 128 * (block % 2)
            spot = (2 * group + tensor, slice(row, row + 16), slice(col, col + 128))
            layer = 1 - group
            old = (layer, *spot[1:])
            old_m, old_v = (m_in[old], v_in[old]) if tensor else (m_out[old], v_out[old])
            grad = red[group][color][slot, own[color]]
            for mask in range(1, 8):
                grad = grad + got[group][color][slot, 55 + mask]
            moment = BETA1 * old_m + (1.0 - BETA1) * grad
            second = BETA2 * old_v + (1.0 - BETA2) * grad * grad
            m_new[spot] = moment
            v_new[spot] = second
            direction = (moment / CORR_MOM) / (jnp.sqrt(second / CORR_VAR) + EPSILON)
            gat[group][color][slot, own[color]] = direction.astype(BF16)

    def eight(color, near, far):
        return start_of(color, 3) + near * 8 * (1 - 2 * bit(color, 2)) + far * 16 * (1 - 2 * bit(color, 1))

    def gather_copy(group, color, stage, near, far):
        spot = gat[group][color].at[:, pl.ds(eight(color, near, far), 8)]
        return message(group, color, 21 + (near if stage == 1 else 2 + near + 2 * far if stage == 0 else 6), spot, spot,
                       by_core(tp, functools.partial(flip, dp), color, stage))

    def gather_start(group, color):
        for stage in (2, 1, 0):
            gather_copy(group, color, stage, 0, 0).start()

    def gather_near(group, color):
        gather_copy(group, color, 2, 0, 0).wait()
        for stage in (1, 0):
            gather_copy(group, color, stage, 1, 0).start()

    def gather_far(group, color):
        for near in range(2):
            gather_copy(group, color, 1, near, 0).wait()
            gather_copy(group, color, 0, near, 1).start()

    def gather_end(group, color):
        for far in range(2):
            for near in range(2):
                gather_copy(group, color, 0, near, far).wait()

    def write_out(group, color):
        return pltpu.make_async_copy(gat[group][color], n_out[group][color], out_sem.at[group, color])

    def colors(function, *args):
        for color in range(COLORS):
            function(*args[:1], color, *args[1:])

    def take(group, color, stage, part, then):
        reduce_add(group, color, stage, part)
        for number in range(then):
            reduce_send(group, color, stage + 1, number)

    def first_send(group, tensor):
        for part in range(2):
            colors(reduce_send, group, 0, 2 * tensor + part)

    def first_take(group, color, kept):
        take(group, color, 0, kept, 0)
        take(group, color, 0, 2 + kept, 0 if kept else 2)

    def direct_start(group, color):
        for mask in range(1, 8):
            direct_reduce(group, color, mask).start()

    def direct_end(group, color):
        for mask in range(1, 8):
            direct_reduce(group, color, mask).wait()
        update(group, color)
        for mask in range(1, 8):
            direct_gather(group, color, mask).start()

    def direct_gathered(group, color):
        for mask in range(1, 8):
            direct_gather(group, color, mask).wait()
        gather_start(group, color)

    def last_stage(group, color):
        reduce_add(group, color, 2, 0)
        direct_start(group, color)

    def finish(group, color):
        gather_end(group, color)
        write_out(group, color).start()

    def forward(slot):
        return sum(dot(h_buf[:, TILE * q : TILE * (q + 1)], w_buf[slot, q]) for q in QUARTERS).astype(BF16)

    def backward(slot):
        return sum(dot(g_buf[:, TILE * q : TILE * (q + 1)], w_buf[slot, q], 1, 1) for q in QUARTERS)

    x_copy.wait()

    def z0_step(tile, carry):
        slot = take_chunk(0, tile)
        z = forward(slot)
        z0_buf[:, columns(tile)] = z
        a_buf[:, columns(tile)] = gelu(z.astype(F32)).astype(BF16)
        return carry

    lax.fori_loop(0, CHUNKS, z0_step, 0)
    pl.semaphore_wait(barrier, len(greeted) + 1)

    def h_step(n, carry):
        total = None
        for half in range(2):
            slot = take_chunk(1, 2 * n + half)
            for q in QUARTERS:
                at = 2048 * half + TILE * q
                term = dot(a_buf[:, at : at + TILE], w_buf[slot, q])
                total = term if total is None else total + term
        pair_send_tile(0, n, total)
        return carry

    lax.fori_loop(0, 4, h_step, 0)
    wait_pq(p_in, 0)
    split(dot(h_buf[...], pq_buf[0]), hp0)
    load_pq(p_in, 1, 0)
    g_copy.wait()
    wait_pq(q_out, 1)
    split(dot(g_buf[...], pq_buf[1]), gq1)
    load_pq(q_out, 0, 1)
    pair_add(0, h_buf)

    def z1_step(tile, carry):
        slot = take_chunk(2, tile)
        z = forward(slot)
        z1_buf[:, columns(tile)] = z
        project(gelu(z.astype(F32)).astype(BF16), gq1, 0, 0, tile)
        return carry

    lax.fori_loop(0, CHUNKS, z1_step, 0)
    first_send(0, 0)
    wait_pq(p_in, 0)
    split(dot(h_buf[...], pq_buf[0]), hp1)

    def da1_step(tile, carry):
        slot = take_chunk(3, tile)
        d_act = backward(slot)
        dz = (gelu_grad(z1_buf[:, columns(tile)].astype(F32)) * d_act).astype(BF16)
        z1_buf[:, columns(tile)] = dz
        project(dz, hp1, 0, 1, tile)
        return carry

    lax.fori_loop(0, CHUNKS, da1_step, 0)
    first_send(0, 1)

    def b_step(n, carry):
        total = None
        for half in range(2):
            slot = take_chunk(4, 2 * n + half)
            for q in QUARTERS:
                at = 2048 * half + TILE * q
                term = dot(z1_buf[:, at : at + TILE], w_buf[slot, q], 1, 1)
                total = term if total is None else total + term
        pair_send_tile(1, n, total)
        return carry

    lax.fori_loop(0, 4, b_step, 0)
    wait_pq(q_out, 1)
    pair_add(1, g_buf)
    split(dot(g_buf[...], pq_buf[1]), gq0)

    def out_step(tile, carry):
        project(a_buf[:, columns(tile)], gq0, 1, 0, tile)
        return carry

    lax.fori_loop(0, CHUNKS, out_step, 0)
    first_send(1, 0)
    colors(first_take, 0, 0)
    colors(first_take, 0, 1)

    def da0_step(tile, carry):
        slot = take_chunk(5, tile)
        d_act = backward(slot)
        dz = (gelu_grad(z0_buf[:, columns(tile)].astype(F32)) * d_act).astype(BF16)
        project(dz, hp0, 1, 1, tile)
        return carry

    lax.fori_loop(0, CHUNKS, da0_step, 0)

    colors(reduce_send, 1, 0, 2)
    colors(take, 0, 1, 0, 1)
    colors(reduce_send, 1, 0, 3)
    colors(take, 0, 1, 1, 0)
    colors(first_take, 1, 0)
    colors(last_stage, 0)
    colors(first_take, 1, 1)
    colors(take, 1, 1, 0, 1)
    colors(direct_end, 0)
    colors(take, 1, 1, 1, 0)
    colors(direct_gathered, 0)
    colors(last_stage, 1)
    colors(gather_near, 0)
    colors(direct_end, 1)
    colors(gather_far, 0)
    colors(direct_gathered, 1)
    colors(finish, 0)
    colors(gather_near, 1)
    colors(gather_far, 1)
    colors(finish, 1)
    for group in range(2):
        for color in range(COLORS):
            write_out(group, color).wait()


READS = 3
WRITES = 2


def apply_kernel(w_in, w_out, p_in, q_out, m_step, v_step, *rest):
    rest = iter(rest)
    shares = [next(rest) for item in range(6)]
    in_new, out_new, m_in, v_in, m_out, v_out = (next(rest) for item in range(6))
    gat = [next(rest) for item in range(6)]
    (p_buf, q_buf, in_read, out_read, in_write, out_write, n_buf,
     share_sem, basis_sem, read_sem, write_sem) = rest
    tp = lax.axis_index("tp")
    pairs = 2 * CHUNKS

    def tile_of(ref, pair, rows):
        layer = 1 - lax.div(pair, CHUNKS)
        at = pl.ds(pl.multiple_of(TILE * lax.rem(pair, CHUNKS), TILE), TILE)
        return ref.at[layer, at] if rows else ref.at[layer, :, at]

    def read(pair, rows):
        ref, buf = (w_out, out_read) if rows else (w_in, in_read)
        slot = lax.rem(pair, READS)
        return pltpu.make_async_copy(tile_of(ref, pair, rows), buf.at[slot], read_sem.at[rows, slot])

    def write(pair, rows):
        ref, buf = (out_new, out_write) if rows else (in_new, in_write)
        slot = lax.rem(pair, WRITES)
        return pltpu.make_async_copy(buf.at[slot], tile_of(ref, pair, rows), write_sem.at[rows, slot])

    def share_copy(item):
        return pltpu.make_async_copy(shares[item], gat[item], share_sem.at[item])

    def basis_copy(layer, rows):
        ref, buf = (q_out, q_buf) if rows else (p_in, p_buf)
        return pltpu.make_async_copy(ref.at[layer], buf.at[layer], basis_sem.at[layer, rows])

    for group in range(2):
        for color in range(COLORS):
            share_copy(COLORS * group + color).start()
        for rows in (1, 0):
            basis_copy(1 - group, rows).start()
        for pair in range(1 if group == 0 else READS):
            if group == 0 or pair:
                for rows in (1, 0):
                    read(jnp.int32(pair), rows).start()

    for step, in_ref, out_ref in ((m_step, m_in, m_out), (v_step, v_in, v_out)):
        for layer in range(2):
            out_ref[layer] = step[2 - 2 * layer]
            in_ref[layer] = step[3 - 2 * layer]

    def gather(group, tile):
        for lane in range(8):
            lane_bits = step_bits(tile, lane)
            spots = [place(lane_bits, color, tp) for color in range(COLORS)]
            for tensor in range(2):
                for block in range(8):
                    color, slot = WHERE[group][tensor, block]
                    row, col = 64 * lane + 16 * (block // 2), 128 * (block % 2)
                    n_buf[tensor, row : row + 16, col : col + 128] = gat[COLORS * group + color][slot, spots[color]]

    def one(pair, carry):
        layer = 1 - lax.div(pair, CHUNKS)
        for group in range(2):

            @pl.when(pair == CHUNKS * group)
            def _():
                for color in range(COLORS):
                    share_copy(COLORS * group + color).wait()
                for rows in (1, 0):
                    basis_copy(1 - group, rows).wait()

            @pl.when(layer == 1 - group)
            def _():
                gather(group, lax.rem(pair, CHUNKS))

        for rows in (1, 0):
            source, target = (out_read, out_write) if rows else (in_read, in_write)
            read(pair, rows).wait()

            @pl.when(pair >= WRITES)
            def _():
                write(pair - WRITES, rows).wait()

            slot, to = lax.rem(pair, READS), lax.rem(pair, WRITES)
            for cut in QUARTERS:
                at = slice(TILE * cut, TILE * (cut + 1))
                if rows:
                    spot = (slice(None), at)
                    change = dot(n_buf[0], q_buf[layer, at, :], 1, 1)
                else:
                    spot = (at, slice(None))
                    change = dot(p_buf[layer, at, :], n_buf[1], 1, 1)
                target[(to, *spot)] = (source[(slot, *spot)].astype(F32) - STEP_SIZE * change).astype(BF16)
            write(pair, rows).start()

            @pl.when(pair + READS < pairs)
            def _():
                read(pair + READS, rows).start()

        return carry

    lax.fori_loop(0, pairs, one, 0)
    for back in range(WRITES):
        for rows in (1, 0):
            write(jnp.int32(pairs - WRITES + back), rows).wait()


def local_step(x_rows, g_rows, w_in, w_out, p_in, q_out, m_in, v_in, m_out, v_out):
    m_in, v_in = (jnp.swapaxes(moment, 1, 2) for moment in (m_in, v_in))
    any_spec = pl.BlockSpec(memory_space=pl.ANY)
    vmem_spec = pl.BlockSpec(memory_space=pltpu.VMEM)
    shares = [jax.ShapeDtypeStruct((len(items), DP, 16, 128), BF16) for colors in BLOCKS for items in colors]
    moments = jax.ShapeDtypeStruct((4, 64, RANK), F32)
    rows_buf, wide_buf = pltpu.VMEM((TOK, D), BF16), pltpu.VMEM((TOK, F), BF16)
    parts_buf = pltpu.VMEM((TOK, 3 * RANK), BF16)
    basis_buf = pltpu.VMEM((2, D, RANK), BF16)
    dma = pltpu.SemaphoreType.DMA
    results = pl.pallas_call(
        step_kernel,
        out_shape=shares + [moments, moments],
        in_specs=[any_spec] * 6 + [vmem_spec] * 4,
        out_specs=[any_spec] * 6 + [vmem_spec] * 2,
        scratch_shapes=[pltpu.VMEM(s.shape, F32) for s in shares]
        + [pltpu.VMEM((s.shape[0], DP - 1, 16, 128), F32) for s in shares]
        + [pltpu.VMEM(s.shape, BF16) for s in shares]
        + [rows_buf] * 2
        + [wide_buf] * 3
        + [pltpu.VMEM((SLOTS, 4, TILE, TILE), BF16), basis_buf]
        + [parts_buf] * 4
        + [dma((SLOTS,)), dma((2,)), dma((2,)), dma((2, 3)), dma((2, 4)), dma((2, 4)), dma((2, 3, 28)), dma((2, 3, 28))],
        compiler_params=pltpu.CompilerParams(
            collective_id=0, has_side_effects=True, vmem_limit_bytes=67_000_000),
        name="galore_step",
    )(x_rows, g_rows, w_in, w_out, p_in, q_out, m_in, v_in, m_out, v_out)
    in_tile, out_tile = (D, TILE), (TILE, D)
    w_in_new, w_out_new, m_in, v_in, m_out, v_out = pl.pallas_call(
        apply_kernel,
        out_shape=[jax.ShapeDtypeStruct(w.shape, w.dtype) for w in (w_in, w_out, m_in, v_in, m_out, v_out)],
        in_specs=[any_spec] * 4 + [vmem_spec] * 2 + [any_spec] * 6,
        out_specs=[any_spec] * 2 + [vmem_spec] * 4,
        scratch_shapes=[pltpu.VMEM(s.shape, BF16) for s in shares]
        + [basis_buf] * 2
        + [pltpu.VMEM((READS, *in_tile), BF16), pltpu.VMEM((READS, *out_tile), BF16)]
        + [pltpu.VMEM((WRITES, *in_tile), BF16), pltpu.VMEM((WRITES, *out_tile), BF16)]
        + [pltpu.VMEM((2, TILE, RANK), BF16), dma((6,)), dma((2, 2)), dma((2, READS)), dma((2, WRITES))],
        compiler_params=pltpu.CompilerParams(vmem_limit_bytes=60_000_000),
        name="galore_apply",
    )(w_in, w_out, p_in, q_out, *results[6:], *results[:6])
    m_in, v_in = (jnp.swapaxes(moment, 1, 2) for moment in (m_in, v_in))
    return w_in_new, w_out_new, m_in, v_in, m_out, v_out


def solution(mesh):
    weight_in_spec = P(None, None, "tp")
    weight_out_spec = P(None, "tp", None)
    moment_in_spec = P(None, None, ("tp", "dp"))
    moment_out_spec = P(None, ("tp", "dp"), None)
    return jax.shard_map(
        local_step,
        mesh=mesh,
        in_specs=(P("dp", None), P("dp", None), weight_in_spec, weight_out_spec, P(), P(),
                  moment_in_spec, moment_in_spec, moment_out_spec, moment_out_spec),
        out_specs=(weight_in_spec, weight_out_spec, moment_in_spec, moment_in_spec, moment_out_spec, moment_out_spec),
        check_vma=False,
    )
```
